32 devices in a mesh: col: 8 (over z, x), row: 4 (over y, core).
Axes of the slice: x: 2, y: 2, z: 4, core: 2. Of those that a mesh axis runs over, the one named last changes fastest.
Arguments:
- vorticity: float32 [2, 8, 1024, 2048], P(None, 'row', 'col'), may hold values from -0.0017578125 to 0.0017578125
- divergence: float32 [2, 8, 1024, 2048], P(None, 'row', 'col'), may hold values from -0.0017578125 to 0.0017578125
- trunc_cut: int32 [1024], P('col'), may hold values from -1 to 1023, as said below
- level_slot: int32 [8], replicated, may hold values from 0 to 7, each once
Outputs:
- u_wind: float32 [8, 2048, 2048], P(None, ('col', 'row'))
- v_wind: float32 [8, 2048, 2048], P(None, ('col', 'row'))
- u_slope: float32 [8, 2048, 2048], P(None, ('col', 'row'))
- v_slope: float32 [8, 2048, 2048], P(None, ('col', 'row'))
The draws below stay inside these ranges and needn't reach their ends.
Inputs may be any that keep to these rules, and one draw needn't show every extreme that they name: trunc_cut never rises with m, is 1023 at m = 0 and -1 (nothing kept) at the last m. level_slot is a permutation of the model levels.
All inputs are finite; a program needn't handle non-finite values.
Results may differ from the reference program's by a relative error of at most 0.0001.
Values sent between devices are 32-bit elements; how exact they have to be, the bound alone decides.
A program may use at most 128 MiB of HBM per device.

```python
import math
import jax
import jax.numpy as jnp
from jax import lax

NX = 2048
NY = 2048
MX = 1024
LEVELS = 8


def draw_trunc_cut(key, part):
    first_key = jax.random.fold_in(key, 11)
    second_key = jax.random.fold_in(key, 23)
    wave_axis = jax.random.randint(first_key, (), 3 * MX // 4, MX - 1)
    north_axis = jax.random.randint(second_key, (), 3 * (NY // 2) // 4, NY // 2)
    wave_index = jnp.arange(MX, dtype=jnp.int32)
    north_index = jnp.arange(NY // 2, dtype=jnp.int32)
    scaled = wave_index * north_axis // wave_axis
    inside = north_index[None, :] * north_index[None, :] + scaled[:, None] * scaled[:, None] <= north_axis * north_axis
    counted = jnp.sum(inside.astype(jnp.int32), axis=1) - 1
    shaped = jnp.where(wave_index > wave_axis, -1, counted)
    return jnp.where(wave_index == 0, NY // 2 - 1, shaped).astype(jnp.int32)


def level_of(stream_key, dims, split, low, top_value):
    gain, own = 1.0, jax.random.fold_in(stream_key, 6)
    for axis_at, blocks in split:
        draws = jnp.exp(jax.random.uniform(jax.random.fold_in(own, axis_at), (blocks,), jnp.float32, low / len(split), top_value / len(split)))
        gain = gain * jnp.repeat(draws, dims[axis_at] // blocks).reshape([-1 if axis == axis_at else 1 for axis in range(len(dims))])
    return gain


def centred(rng, dims, deviation, bound, shards=(), kind=jnp.bfloat16):
    gain = level_of(rng, dims, shards, -0.22, 0.18) if shards else 1.0
    drawn = jax.random.normal(rng, dims, jnp.float32) * deviation * gain
    return jnp.minimum(jnp.maximum(drawn, -bound), bound).astype(kind)


def setup_inputs(seed: int = 0) -> dict:
    key_of = jax.random.split(jax.random.key(seed), 5)
    return {
        "vorticity": centred(key_of[0], (2, LEVELS, MX, NY), (0.6 * NX ** -1), 0.0017578125, ((1, 4), (2, 8)), jnp.float32),
        "divergence": centred(key_of[1], (2, LEVELS, MX, NY), (0.6 * NX ** -1), 0.0017578125, ((1, 4), (2, 8)), jnp.float32),
        "trunc_cut": draw_trunc_cut(jax.random.fold_in(key_of[4], 71), 0),
        "level_slot": jax.random.permutation(key_of[3], LEVELS).astype(jnp.int32),
    }


def reference(vorticity, divergence, trunc_cut, level_slot):
    wave_index = jnp.arange(NX // 2, dtype=jnp.int32)
    north_index = jnp.arange(NY, dtype=jnp.int32)
    north_wave = jnp.where(north_index < NY // 2, north_index, north_index - NY)
    wave_east = (2.0 * math.pi / NX) * wave_index.astype(jnp.float32)
    wave_north = (2.0 * math.pi / NY) * north_wave.astype(jnp.float32)
    east_col = wave_east[:, None]
    north_row = wave_north[None, :]
    square_wave = east_col * east_col + north_row * north_row
    retained = (jnp.abs(north_wave)[None, :] <= trunc_cut[:, None]) & (square_wave > 0)
    inverse_square = jnp.where(retained, 1.0 / jnp.where(square_wave > 0, square_wave, 1.0), 0.0)
    weights = jnp.where(wave_index == 0, 1.0, 2.0).astype(jnp.float32)

    def one_level(slot_data):
        curl_real, curl_imag, source_real, source_imag = slot_data
        east_real = (-north_row * curl_imag + east_col * source_imag) * inverse_square
        east_imag = (north_row * curl_real - east_col * source_real) * inverse_square
        north_real = (east_col * curl_imag + north_row * source_imag) * inverse_square
        north_imag = (-east_col * curl_real - north_row * source_real) * inverse_square
        results = []
        for real_part, imag_part in ((east_real, east_imag), (north_real, north_imag)):
            coeffs = real_part + 1j * imag_part
            meridional = jnp.fft.ifft(coeffs, axis=1) * NY
            weighted = meridional * weights[:, None]
            padded = jnp.concatenate([weighted, jnp.zeros_like(weighted)], axis=0)
            value_grid = (jnp.fft.ifft(padded, axis=0) * NX).real.T
            sloped = jnp.concatenate([weighted * (1j * wave_east[:, None]), jnp.zeros_like(weighted)], axis=0)
            slope_grid = (jnp.fft.ifft(sloped, axis=0) * NX).real.T
            results.append(value_grid)
            results.append(slope_grid)
        return tuple(results)

    values = lax.map(one_level, (vorticity[0], vorticity[1], divergence[0], divergence[1]))
    inverse = jnp.argsort(level_slot).astype(jnp.int32)
    return (values[0][inverse], values[2][inverse], values[1][inverse], values[3][inverse])
```

```python
import functools
import math

import jax
import jax.numpy as jnp
import numpy as np
from jax import lax
from jax.experimental import pallas as pl
from jax.experimental.pallas import tpu as pltpu
from jax.sharding import PartitionSpec as P

MESH = pl.DeviceIdType.MESH
LANES = 128
ROWS = 16
FINE = 32
HIGH = lax.Precision.HIGH


def split_waves(array, axis):
    first = lax.slice_in_dim(array, 0, None, 2, axis)
    second = lax.slice_in_dim(array, 1, None, 2, axis)
    return jnp.concatenate([first, second], axis)


def phases(product, period):
    angles = 2.0 * np.pi * (product % period) / period
    return np.cos(angles).astype(np.float32), np.sin(angles).astype(np.float32)


def multiply(first, second):
    return first[0] * second[0] - first[1] * second[1], first[0] * second[1] + first[1] * second[0]


def north_table(north_cells):
    quarter = north_cells // 4
    fine = math.gcd(quarter, 32)
    column = np.arange(quarter)
    coarse_row = 4 * fine * np.arange(quarter // fine)[None, :, None, None] + np.arange(4)[:, None, None, None]
    fine_row = 4 * np.arange(fine)[None, None, :, None]
    coarse = phases(coarse_row * column, north_cells)
    close = phases(fine_row * column, north_cells)
    coarse, close = lax.optimization_barrier((coarse, close))
    cosine, sine = multiply(coarse, close)
    joined = jnp.concatenate([cosine, -sine], axis=3)
    return joined.reshape(4, quarter, 2 * quarter)


def east_table(columns, local_waves, east_cells):
    half = local_waves // 2
    cells = east_cells // 2
    column = np.arange(cells)
    coarse_wave = np.arange(2)[:, None, None, None] + local_waves * np.arange(columns)[None, :, None, None]
    close_wave = 2 * np.arange(half)[None, None, :, None]
    coarse = phases(coarse_wave * column, east_cells)
    close = phases(close_wave * column, east_cells)
    coarse, close = lax.optimization_barrier((coarse, close))
    cosine, sine = multiply(coarse, close)
    wave = coarse_wave + close_wave
    weights = np.where(wave == 0, 1.0, 2.0).astype(np.float32)
    scaled = (weights * wave * (2.0 * np.pi / east_cells)).astype(np.float32)
    real = jnp.concatenate([weights * cosine, -scaled * sine], axis=3)
    imag = jnp.concatenate([-weights * sine, -scaled * cosine], axis=3)
    joined = jnp.stack([real, imag], axis=2)
    return joined.reshape(2, columns * local_waves, 2 * cells)


def spectral_winds(vorticity, divergence, trunc_cut, wave_index, east_cells):
    north_cells = vorticity.shape[3]
    north_index = jnp.arange(north_cells, dtype=jnp.int32)
    north_wave = jnp.where(north_index < north_cells // 2, north_index, north_index - north_cells)
    wave_east = 2.0 * math.pi / east_cells * wave_index.astype(jnp.float32)
    wave_north = 2.0 * math.pi / north_cells * north_wave.astype(jnp.float32)
    east_col = wave_east[:, None]
    north_row = wave_north[None, :]
    square_wave = east_col * east_col + north_row * north_row
    retained = (jnp.abs(north_wave)[None, :] <= trunc_cut[:, None]) & (square_wave > 0)
    inverse_square = jnp.where(retained, 1.0 / jnp.where(square_wave > 0, square_wave, 1.0), 0.0)
    east_inverse = east_col * inverse_square
    north_inverse = north_row * inverse_square
    curl_real, curl_imag = vorticity[0], vorticity[1]
    source_real, source_imag = divergence[0], divergence[1]
    east = (
        -north_inverse * curl_imag + east_inverse * source_imag,
        north_inverse * curl_real - east_inverse * source_real,
    )
    north = (
        east_inverse * curl_imag + north_inverse * source_imag,
        -east_inverse * curl_real - north_inverse * source_real,
    )
    return east, north


def fold_quarters(wind, slots, half):
    real, imag = wind
    quarter = real.shape[2] // 4
    r0, r1, r2, r3 = (real[:, :, q * quarter:(q + 1) * quarter] for q in range(4))
    i0, i1, i2, i3 = (imag[:, :, q * quarter:(q + 1) * quarter] for q in range(4))
    folded = (
        (r0 + r2 + (r1 + r3), i0 + i2 + (i1 + i3)),
        (r0 - r2 - (i1 - i3), i0 - i2 + (r1 - r3)),
        (r0 + r2 - (r1 + r3), i0 + i2 - (i1 + i3)),
        (r0 - r2 + (i1 - i3), i0 - i2 - (r1 - r3)),
    )
    parts = []
    for part_real, part_imag in folded:
        shape = (slots, 2, 1, half, 2 * quarter)
        top = jnp.concatenate([part_real, part_imag], axis=2).reshape(shape)
        low = jnp.concatenate([part_imag, -part_real], axis=2).reshape(shape)
        parts.append(jnp.concatenate([top, low], axis=2))
    return jnp.stack(parts, axis=0).reshape(4, slots * 4 * half, 2 * quarter)


def general_device(vorticity, divergence, trunc_cut, level_slot):
    columns = lax.axis_size("col")
    row_devices = lax.axis_size("row")
    slots, local_waves, north_cells = vorticity.shape[1:]
    half = local_waves // 2
    quarter = north_cells // 4
    levels = slots * row_devices
    east_cells = 2 * local_waves * columns
    cells = east_cells // 2
    block = quarter // (columns * row_devices)
    first_wave = lax.axis_index("col") * local_waves
    wave_index = first_wave + jnp.arange(local_waves, dtype=jnp.int32)
    winds = spectral_winds(
        split_waves(vorticity, 2),
        split_waves(divergence, 2),
        split_waves(trunc_cut, 0),
        split_waves(wave_index, 0),
        east_cells,
    )
    table_north = north_table(north_cells)
    table_east = east_table(columns, local_waves, east_cells)
    holder = jnp.argsort(level_slot).astype(jnp.int32)
    results = []
    for wind in winds:
        folded = fold_quarters(wind, slots, half)
        fourier = jnp.einsum("pjk,pmk->pjm", table_north, folded, precision=HIGH)
        outgoing = fourier.reshape(4, quarter, slots, 2 * local_waves).transpose(1, 2, 0, 3)
        received = lax.all_to_all(outgoing, ("col", "row"), split_axis=0, concat_axis=0, tiled=True)
        shaped = received.reshape(columns, row_devices, block, slots, 4, 2, local_waves)
        arranged = shaped.transpose(1, 3, 5, 2, 4, 0, 6).reshape(
            levels, 2, block * 4, columns * local_waves
        )
        placed = jnp.concatenate(
            [lax.dynamic_slice_in_dim(arranged, holder[level], 1, 0) for level in range(levels)], axis=0
        )
        even = jnp.einsum("lyk,kx->lyx", placed[:, 0], table_east[0], precision=HIGH)
        odd = jnp.einsum("lyk,kx->lyx", placed[:, 1], table_east[1], precision=HIGH)
        total, rest = even + odd, even - odd
        results.append(
            (
                jnp.concatenate([total[:, :, :cells], rest[:, :, :cells]], axis=2),
                jnp.concatenate([total[:, :, cells:], rest[:, :, cells:]], axis=2),
            )
        )
    return results[0][0], results[1][0], results[0][1], results[1][1]


def cos_sin(product, period):
    angles = 2.0 * np.pi * (product % period) / period
    return np.stack([np.cos(angles), np.sin(angles)]).astype(np.float32)


def split(value):
    high = value.astype(jnp.bfloat16)
    return high, (value - high.astype(jnp.float32)).astype(jnp.bfloat16)


def dot3(left, right, dims):
    def one(first, second):
        return lax.dot_general(first, second, (dims, ((), ())), preferred_element_type=jnp.float32)

    return one(left[0], right[0]) + one(left[0], right[1]) + one(left[1], right[0])


def sizes_of(shape, columns, row_devices):
    slots, local, north_cells = shape[1:]
    return dict(
        columns=columns,
        rows=row_devices,
        devices=columns * row_devices,
        slots=slots,
        local=local,
        half=local // 2,
        north=north_cells,
        quarter=north_cells // 4,
        share=north_cells // (columns * row_devices),
        east=2 * local * columns,
        cells=local * columns,
    )


def build_north_table(sz, fine, coarse, table):
    quarter = sz["quarter"]

    def step(g, carry):
        cos_c, sin_c = coarse[0, pl.ds(g, 1), :], coarse[1, pl.ds(g, 1), :]
        cos_f, sin_f = fine[0], fine[1]
        cosine = cos_c * cos_f - sin_c * sin_f
        sine = -(sin_c * cos_f + cos_c * sin_f)
        at = pl.ds(pl.multiple_of(g * FINE, FINE), FINE)
        for part, value in ((0, cosine), (1, sine)):
            high, low = split(value)
            table[0, at, part * quarter:(part + 1) * quarter] = high
            table[1, at, part * quarter:(part + 1) * quarter] = low
        return carry

    lax.fori_loop(0, quarter // FINE, step, 0)


def build_east_table(sz, fine, coarse, table):
    half, columns, cells = sz["half"], sz["columns"], sz["cells"]
    width = min(cells, 256)

    def step(index, carry):
        parity, column = index // columns, index % columns
        base = column * (2 * half)
        for start in range(0, cells, width):
            lanes = slice(start, start + width)
            cos_c, sin_c = coarse[0, pl.ds(index, 1), lanes], coarse[1, pl.ds(index, 1), lanes]
            cos_f, sin_f = fine[0, :, lanes], fine[1, :, lanes]
            cosine = cos_c * cos_f - sin_c * sin_f
            sine = -(sin_c * cos_f + cos_c * sin_f)
            for part, value in ((0, cosine), (1, sine)):
                at = pl.ds(pl.multiple_of(base + part * half, half), half)
                high, low = split(value)
                table[0, parity, at, lanes] = high
                table[1, parity, at, lanes] = low
        return carry

    lax.fori_loop(0, 2 * columns, step, 0)


def build_folded(sz, slot, wind, column, curl, source, cut, twiddle, folded):
    half, quarter, north = sz["half"], sz["quarter"], sz["north"]
    is_north = wind == 1

    def step(block, carry):
        lanes = pl.multiple_of(block * LANES, LANES)
        index = lax.broadcasted_iota(jnp.int32, (ROWS, LANES), 1) + lanes
        line = lax.broadcasted_iota(jnp.int32, (ROWS, LANES), 0)
        for parity in range(2):
            for top in range(0, half, ROWS):
                at = pl.ds(parity + 2 * top, ROWS, stride=2)
                wave = column * (2 * half) + parity + 2 * (line + top)
                kx = (2.0 * math.pi / sz["east"]) * wave.astype(jnp.float32)
                weight = jnp.where(wave == 0, 1.0, 2.0)
                kept = cut[at, :]
                real, imag = [], []
                for q in range(4):
                    number = index + q * quarter
                    number = jnp.where(number < north // 2, number, number - north)
                    ky = (2.0 * math.pi / north) * number.astype(jnp.float32)
                    square = kx * kx + ky * ky
                    retained = (jnp.abs(number) <= kept) & (square > 0)
                    inverse = jnp.where(retained, weight / jnp.where(square > 0, square, 1.0), 0.0)
                    by_x, by_y = kx * inverse, ky * inverse
                    first = jnp.where(is_north, by_x, -by_y)
                    second = jnp.where(is_north, by_y, by_x)
                    strip = block + q * (quarter // LANES)
                    zr, zi = curl[slot, strip, 0, at, :], curl[slot, strip, 1, at, :]
                    dr, di = source[slot, strip, 0, at, :], source[slot, strip, 1, at, :]
                    real.append(first * zi + second * di)
                    imag.append(-(first * zr + second * dr))
                (r0, r1, r2, r3), (i0, i1, i2, i3) = real, imag
                rs, rd, rt, ru = r0 + r2, r0 - r2, r1 + r3, r1 - r3
                js, jd, jt, ju = i0 + i2, i0 - i2, i1 + i3, i1 - i3
                parts = ((rs + rt, js + jt), (rd - ju, jd + ru), (rs - rt, js - jt), (rd + ju, jd - ru))
                near = pl.ds(lanes, LANES)
                far = pl.ds(pl.multiple_of(lanes + quarter, LANES), LANES)
                for p, (a, b) in enumerate(parts):
                    if p:
                        cosine = twiddle[2 * p:2 * p + 1, near]
                        sine = twiddle[2 * p + 1:2 * p + 2, near]
                        a, b = a * cosine - b * sine, a * sine + b * cosine
                    upper = slice(parity * 2 * half + top, parity * 2 * half + top + ROWS)
                    lower = slice(parity * 2 * half + half + top, parity * 2 * half + half + top + ROWS)
                    for level, (x, y) in enumerate(zip(split(a), split(b))):
                        folded[level, p, upper, near] = x
                        folded[level, p, upper, far] = y
                        folded[level, p, lower, near] = y
                        folded[level, p, lower, far] = -x
        return carry

    lax.fori_loop(0, quarter // LANES, step, 0)


def north_transform(sz, chunk, table, folded, outgoing):
    quarter = sz["quarter"]
    for p in range(4):
        left = (table[0], table[1])
        right = (folded[0, p], folded[1, p])
        sums = dot3(left, right, ((1,), (1,)))
        for parity in range(2):
            outgoing[chunk, parity, pl.ds(p, quarter, stride=4), :] = sums[:, parity * LANES:(parity + 1) * LANES]


def build_waves(sz, received, waves):
    columns, half = sz["columns"], sz["half"]
    lines = sz["rows"] * sz["share"]

    def step(column, carry):
        sources = pl.ds(pl.multiple_of(column * sz["rows"], sz["rows"]), sz["rows"])
        lane = lax.broadcasted_iota(jnp.int32, (1, 2 * half), 1)
        into = pl.ds(pl.multiple_of(column * 2 * half, LANES), 2 * half)
        for parity in range(2):
            value = received[sources, parity].reshape(lines, 2 * half)
            wave = column * (2 * half) + parity + 2 * jnp.where(lane < half, lane, lane - half)
            kx = (2.0 * math.pi / sz["east"]) * wave.astype(jnp.float32)
            slope = pltpu.roll(value, half, axis=1) * jnp.where(lane < half, -kx, kx)
            for kind, data in enumerate((value, slope)):
                high, low = split(data)
                waves[0, parity, kind * lines:(kind + 1) * lines, into] = high
                waves[1, parity, kind * lines:(kind + 1) * lines, into] = low
        return carry

    lax.fori_loop(0, columns, step, 0)


def east_tile(sz, waves, table, lanes):
    sums = []
    for parity in range(2):
        left = (waves[0, parity], waves[1, parity])
        right = (table[0, parity, :, lanes], table[1, parity, :, lanes])
        sums.append(dot3(left, right, ((1,), (0,))))
    return sums[0] + sums[1], sums[0] - sums[1]


def exchange_kernel(
    sz, curl_hbm, source_hbm, cut, fine_north, coarse_north, twiddle, fine_east, coarse_east,
    results, last, table_out,
    curl, source, table_north, table_east, folded, outgoing, incoming, waves, grid,
    load_sem, send_sem, recv_sem, own_sem, out_sem, table_sem,
):
    columns, rows, devices, slots = sz["columns"], sz["rows"], sz["devices"], sz["slots"]
    share, cells = sz["share"], sz["cells"]
    chunks = 2 * slots
    col, row = lax.axis_index("col"), lax.axis_index("row")
    me = col * rows + row
    strips = sz["north"] // LANES

    def load(slot, strip):
        lanes = pl.ds(pl.multiple_of(strip * LANES, LANES), LANES)
        for which, (hbm, near) in enumerate(((curl_hbm, curl), (source_hbm, source))):
            yield pltpu.make_async_copy(
                hbm.at[:, slot, :, lanes], near.at[slot, strip], load_sem.at[which, slot, strip]
            )

    def start_load(index, carry):
        for copy in load(index // strips, index % strips):
            copy.start()
        return carry

    lax.fori_loop(0, slots * strips, start_load, 0)
    barrier = pltpu.get_barrier_semaphore()

    def target(offset):
        there_col = lax.rem(col + offset % columns, columns)
        there_row = lax.rem(row + offset // columns, rows)
        return there_col, there_row

    def origin(offset):
        from_col = lax.rem(col + columns - offset % columns, columns)
        from_row = lax.rem(row + rows - offset // columns, rows)
        return from_col * rows + from_row

    def greet(offset, carry):
        pl.semaphore_signal(barrier, inc=1, device_id=target(offset), device_id_type=MESH)
        return carry

    lax.fori_loop(1, devices, greet, 0)
    build_north_table(sz, fine_north, coarse_north, table_north)
    pl.semaphore_wait(barrier, devices - 1)

    def block_of(device):
        return pl.ds(pl.multiple_of(device * share, share), share)

    def send(chunk, offset, slot_ref):
        there_col, there_row = target(offset)
        return pltpu.make_async_remote_copy(
            src_ref=outgoing.at[chunk, :, block_of(there_col * rows + there_row)],
            dst_ref=slot_ref,
            send_sem=send_sem.at[chunk, offset],
            recv_sem=recv_sem.at[chunk, offset],
            device_id=(there_col, there_row),
            device_id_type=MESH,
        )

    def own(chunk, slot_ref):
        return pltpu.make_async_copy(outgoing.at[chunk, :, block_of(me)], slot_ref, own_sem.at[chunk])

    def launch(chunk, arrivals):
        own(chunk, arrivals(me)).start()

        def step(offset, carry):
            send(chunk, offset, arrivals(me)).start()
            return carry

        lax.fori_loop(1, devices, step, 0)

    def collect(chunk, arrivals):
        own(chunk, arrivals(me)).wait()

        def step(offset, carry):
            send(chunk, offset, arrivals(origin(offset))).wait_recv()
            return carry

        lax.fori_loop(1, devices, step, 0)

    def drain(chunk, arrivals):
        def step(offset, carry):
            send(chunk, offset, arrivals(me)).wait_send()
            return carry

        lax.fori_loop(1, devices, step, 0)

    def produce(chunk, carry):
        slot, wind = chunk // 2, chunk % 2
        @pl.when(wind == 0)
        def _():
            def wait_load(strip, inner):
                for copy in load(slot, strip):
                    copy.wait()
                return inner

            lax.fori_loop(0, strips, wait_load, 0)

        build_folded(sz, slot, wind, col, curl, source, cut, twiddle, folded)
        north_transform(sz, chunk, table_north, folded, outgoing)

        @pl.when(chunk < chunks - 1)
        def _():
            launch(chunk, lambda device: incoming.at[chunk, device])

        @pl.when(chunk == chunks - 1)
        def _():
            launch(chunk, lambda device: last.at[device])

        return carry

    lax.fori_loop(0, chunks, produce, 0)
    build_east_table(sz, fine_east, coarse_east, table_east)
    table_copy = pltpu.make_async_copy(table_east, table_out, table_sem)
    table_copy.start()

    def result_copy(chunk):
        return pltpu.make_async_copy(grid, results.at[chunk], out_sem)

    def consume(chunk, carry):
        collect(chunk, lambda device: incoming.at[chunk, device])
        build_waves(sz, incoming.at[chunk], waves)

        @pl.when(chunk > 0)
        def _():
            result_copy(chunk - 1).wait()

        def tile(index, inner):
            at = pl.multiple_of(index * 256, 256)
            total, rest = east_tile(sz, waves, table_east, pl.ds(at, 256))
            grid[:, pl.ds(at, 256)] = total
            grid[:, pl.ds(pl.multiple_of(at + cells, 256), 256)] = rest
            return inner

        lax.fori_loop(0, cells // 256, tile, 0)
        result_copy(chunk).start()
        return carry

    lax.fori_loop(0, chunks - 1, consume, 0)
    result_copy(chunks - 2).wait()
    table_copy.wait()

    def drain_early(chunk, carry):
        drain(chunk, lambda device: incoming.at[chunk, device])
        return carry

    lax.fori_loop(0, chunks - 1, drain_early, 0)
    collect(chunks - 1, lambda device: last.at[device])
    drain(chunks - 1, lambda device: last.at[device])


def finish_kernel(
    sz, level_slot, results, last, table, u_wind, v_wind, u_slope, v_slope,
    arrived, east, waves, grid, stage, arrive_sem, table_sem, stage_sem, place_sem, write_sem,
):
    rows, slots, share, cells = sz["rows"], sz["slots"], sz["share"], sz["cells"]
    chunks = 2 * slots
    outs = ((u_wind, v_wind), (u_slope, v_slope))
    tiles = cells // 256
    arrive = pltpu.make_async_copy(last, arrived, arrive_sem)
    arrive.start()
    tables = []
    for t in range(tiles):
        at = pl.ds(t * 256, 256)
        copy = pltpu.make_async_copy(table.at[:, :, :, at], east.at[:, :, :, at], table_sem.at[t])
        copy.start()
        tables.append(copy)
    staged = []
    for chunk in range(chunks - 1):
        copy = pltpu.make_async_copy(results.at[chunk], stage.at[chunk], stage_sem.at[chunk])
        copy.start()
        staged.append(copy)

    def level_of(row, slot):
        return level_slot[row * slots + slot]

    pending = []

    def place(chunk):
        staged[chunk].wait()
        for kind in range(2):
            for row in range(rows):
                lines = pl.ds((kind * rows + row) * share, share)
                copy = pltpu.make_async_copy(
                    stage.at[chunk, lines],
                    outs[kind][chunk % 2].at[level_of(row, chunk // 2)],
                    place_sem.at[chunk, kind * rows + row],
                )
                copy.start()
                pending.append(copy)

    arrive.wait()
    build_waves(sz, arrived, waves)
    for t in range(tiles):
        tables[t].wait()
        total, rest = east_tile(sz, waves, east, pl.ds(t * 256, 256))
        grid[:, t * 256:(t + 1) * 256] = total
        grid[:, cells + t * 256:cells + (t + 1) * 256] = rest
        for part, start in enumerate((t * 256, cells + t * 256)):
            for kind in range(2):
                for row in range(rows):
                    lines = pl.ds((kind * rows + row) * share, share)
                    copy = pltpu.make_async_copy(
                        grid.at[lines, pl.ds(start, 256)],
                        outs[kind][1].at[level_of(row, slots - 1), :, pl.ds(start, 256)],
                        write_sem.at[t, part, kind * rows + row],
                    )
                    copy.start()
                    pending.append(copy)
        if t < chunks - 1:
            place(t)
    for chunk in range(tiles, chunks - 1):
        place(chunk)
    for copy in pending:
        copy.wait()


def on_device(vorticity, divergence, trunc_cut, level_slot):
    columns, row_devices = lax.axis_size("col"), lax.axis_size("row")
    sz = sizes_of(vorticity.shape, columns, row_devices)
    if sz["local"] != LANES or sz["cells"] % 256 or sz["quarter"] % LANES:
        return general_device(vorticity, divergence, trunc_cut, level_slot)
    local, half, quarter, cells = sz["local"], sz["half"], sz["quarter"], sz["cells"]
    devices, slots, share, east = sz["devices"], sz["slots"], sz["share"], sz["east"]
    chunks, levels = 2 * slots, slots * row_devices
    strips = sz["north"] // LANES
    lines = 2 * row_devices * share
    column = np.arange(quarter)
    fine_north = cos_sin(np.arange(FINE)[:, None] * column, quarter)
    coarse_north = cos_sin(FINE * np.arange(quarter // FINE)[:, None] * column, quarter)
    twiddle = cos_sin(np.arange(4)[:, None] * column, sz["north"]).transpose(1, 0, 2).reshape(8, quarter)
    cell = np.arange(cells)
    fine_east = cos_sin(2 * np.arange(half)[:, None] * cell, east)
    first = np.arange(2)[:, None] + local * np.arange(columns)[None, :]
    coarse_east = cos_sin(first.reshape(-1, 1) * cell, east)
    cut = jnp.broadcast_to(trunc_cut[:, None], (local, LANES))
    f32, bf16 = jnp.float32, jnp.bfloat16
    anywhere = pl.BlockSpec(memory_space=pl.ANY)
    here = pl.BlockSpec(memory_space=pltpu.VMEM)
    results, last, table = pl.pallas_call(
        functools.partial(exchange_kernel, sz),
        out_shape=(
            jax.ShapeDtypeStruct((chunks - 1, lines, east), f32),
            jax.ShapeDtypeStruct((devices, 2, share, local), f32),
            jax.ShapeDtypeStruct((2, 2, cells, cells), bf16),
        ),
        in_specs=[anywhere] * 2 + [here] * 6,
        out_specs=(anywhere,) * 3,
        scratch_shapes=[
            pltpu.VMEM((slots, strips, 2, local, LANES), f32),
            pltpu.VMEM((slots, strips, 2, local, LANES), f32),
            pltpu.VMEM((2, quarter, 2 * quarter), bf16),
            pltpu.VMEM((2, 2, cells, cells), bf16),
            pltpu.VMEM((2, 4, 2 * local, 2 * quarter), bf16),
            pltpu.VMEM((chunks, 2, sz["north"], local), f32),
            pltpu.VMEM((chunks - 1, devices, 2, share, local), f32),
            pltpu.VMEM((2, 2, lines, cells), bf16),
            pltpu.VMEM((lines, east), f32),
            pltpu.SemaphoreType.DMA((2, slots, strips)),
            pltpu.SemaphoreType.DMA((chunks, devices)),
            pltpu.SemaphoreType.DMA((chunks, devices)),
            pltpu.SemaphoreType.DMA((chunks,)),
            pltpu.SemaphoreType.DMA,
            pltpu.SemaphoreType.DMA,
        ],
        compiler_params=pltpu.CompilerParams(
            collective_id=0, has_side_effects=True, vmem_limit_bytes=60 * 1024 * 1024
        ),
        name="exchange",
    )(vorticity, divergence, cut, fine_north, coarse_north, twiddle, fine_east, coarse_east)
    out = jax.ShapeDtypeStruct((levels, share, east), f32)
    return pl.pallas_call(
        functools.partial(finish_kernel, sz),
        out_shape=(out,) * 4,
        in_specs=[pl.BlockSpec(memory_space=pltpu.SMEM)] + [anywhere] * 3,
        out_specs=(anywhere,) * 4,
        scratch_shapes=[
            pltpu.VMEM((devices, 2, share, local), f32),
            pltpu.VMEM((2, 2, cells, cells), bf16),
            pltpu.VMEM((2, 2, lines, cells), bf16),
            pltpu.VMEM((lines, east), f32),
            pltpu.VMEM((chunks - 1, lines, east), f32),
            pltpu.SemaphoreType.DMA,
            pltpu.SemaphoreType.DMA((cells // 256,)),
            pltpu.SemaphoreType.DMA((chunks - 1,)),
            pltpu.SemaphoreType.DMA((chunks - 1, 2 * row_devices)),
            pltpu.SemaphoreType.DMA((cells // 256, 2, 2 * row_devices)),
        ],
        compiler_params=pltpu.CompilerParams(vmem_limit_bytes=60 * 1024 * 1024),
        name="finish",
    )(level_slot, results, last, table)


def solution(mesh):
    return jax.shard_map(
        on_device,
        mesh=mesh,
        in_specs=(P(None, "row", "col", None), P(None, "row", "col", None), P("col"), P()),
        out_specs=(P(None, ("col", "row"), None),) * 4,
        check_vma=False,
    )
```

```python
import functools
import math

import jax
import jax.numpy as jnp
import numpy as np
from jax import lax
from jax.experimental import pallas as pl
from jax.experimental.pallas import tpu as pltpu
from jax.sharding import PartitionSpec as P

MESH = pl.DeviceIdType.MESH
LANES = 128
ROWS = 16
FINE = 32
TILE = 256
HIGH = lax.Precision.HIGH


def split_waves(array, axis):
    first = lax.slice_in_dim(array, 0, None, 2, axis)
    second = lax.slice_in_dim(array, 1, None, 2, axis)
    return jnp.concatenate([first, second], axis)


def phases(product, period):
    angles = 2.0 * np.pi * (product % period) / period
    return np.cos(angles).astype(np.float32), np.sin(angles).astype(np.float32)


def multiply(first, second):
    return first[0] * second[0] - first[1] * second[1], first[0] * second[1] + first[1] * second[0]


def north_table(north_cells):
    quarter = north_cells // 4
    fine = math.gcd(quarter, 32)
    column = np.arange(quarter)
    coarse_row = 4 * fine * np.arange(quarter // fine)[None, :, None, None] + np.arange(4)[:, None, None, None]
    fine_row = 4 * np.arange(fine)[None, None, :, None]
    coarse = phases(coarse_row * column, north_cells)
    close = phases(fine_row * column, north_cells)
    coarse, close = lax.optimization_barrier((coarse, close))
    cosine, sine = multiply(coarse, close)
    joined = jnp.concatenate([cosine, -sine], axis=3)
    return joined.reshape(4, quarter, 2 * quarter)


def east_table(columns, local_waves, east_cells):
    half = local_waves // 2
    cells = east_cells // 2
    column = np.arange(cells)
    coarse_wave = np.arange(2)[:, None, None, None] + local_waves * np.arange(columns)[None, :, None, None]
    close_wave = 2 * np.arange(half)[None, None, :, None]
    coarse = phases(coarse_wave * column, east_cells)
    close = phases(close_wave * column, east_cells)
    coarse, close = lax.optimization_barrier((coarse, close))
    cosine, sine = multiply(coarse, close)
    wave = coarse_wave + close_wave
    weights = np.where(wave == 0, 1.0, 2.0).astype(np.float32)
    scaled = (weights * wave * (2.0 * np.pi / east_cells)).astype(np.float32)
    real = jnp.concatenate([weights * cosine, -scaled * sine], axis=3)
    imag = jnp.concatenate([-weights * sine, -scaled * cosine], axis=3)
    joined = jnp.stack([real, imag], axis=2)
    return joined.reshape(2, columns * local_waves, 2 * cells)


def spectral_winds(vorticity, divergence, trunc_cut, wave_index, east_cells):
    north_cells = vorticity.shape[3]
    north_index = jnp.arange(north_cells, dtype=jnp.int32)
    north_wave = jnp.where(north_index < north_cells // 2, north_index, north_index - north_cells)
    wave_east = 2.0 * math.pi / east_cells * wave_index.astype(jnp.float32)
    wave_north = 2.0 * math.pi / north_cells * north_wave.astype(jnp.float32)
    east_col = wave_east[:, None]
    north_row = wave_north[None, :]
    square_wave = east_col * east_col + north_row * north_row
    retained = (jnp.abs(north_wave)[None, :] <= trunc_cut[:, None]) & (square_wave > 0)
    inverse_square = jnp.where(retained, 1.0 / jnp.where(square_wave > 0, square_wave, 1.0), 0.0)
    east_inverse = east_col * inverse_square
    north_inverse = north_row * inverse_square
    curl_real, curl_imag = vorticity[0], vorticity[1]
    source_real, source_imag = divergence[0], divergence[1]
    east = (
        -north_inverse * curl_imag + east_inverse * source_imag,
        north_inverse * curl_real - east_inverse * source_real,
    )
    north = (
        east_inverse * curl_imag + north_inverse * source_imag,
        -east_inverse * curl_real - north_inverse * source_real,
    )
    return east, north


def fold_quarters(wind, slots, half):
    real, imag = wind
    quarter = real.shape[2] // 4
    r0, r1, r2, r3 = (real[:, :, q * quarter:(q + 1) * quarter] for q in range(4))
    i0, i1, i2, i3 = (imag[:, :, q * quarter:(q + 1) * quarter] for q in range(4))
    folded = (
        (r0 + r2 + (r1 + r3), i0 + i2 + (i1 + i3)),
        (r0 - r2 - (i1 - i3), i0 - i2 + (r1 - r3)),
        (r0 + r2 - (r1 + r3), i0 + i2 - (i1 + i3)),
        (r0 - r2 + (i1 - i3), i0 - i2 - (r1 - r3)),
    )
    parts = []
    for part_real, part_imag in folded:
        shape = (slots, 2, 1, half, 2 * quarter)
        top = jnp.concatenate([part_real, part_imag], axis=2).reshape(shape)
        low = jnp.concatenate([part_imag, -part_real], axis=2).reshape(shape)
        parts.append(jnp.concatenate([top, low], axis=2))
    return jnp.stack(parts, axis=0).reshape(4, slots * 4 * half, 2 * quarter)


def general_device(vorticity, divergence, trunc_cut, level_slot):
    columns = lax.axis_size("col")
    row_devices = lax.axis_size("row")
    slots, local_waves, north_cells = vorticity.shape[1:]
    half = local_waves // 2
    quarter = north_cells // 4
    levels = slots * row_devices
    east_cells = 2 * local_waves * columns
    cells = east_cells // 2
    block = quarter // (columns * row_devices)
    first_wave = lax.axis_index("col") * local_waves
    wave_index = first_wave + jnp.arange(local_waves, dtype=jnp.int32)
    winds = spectral_winds(
        split_waves(vorticity, 2),
        split_waves(divergence, 2),
        split_waves(trunc_cut, 0),
        split_waves(wave_index, 0),
        east_cells,
    )
    table_north = north_table(north_cells)
    table_east = east_table(columns, local_waves, east_cells)
    holder = jnp.argsort(level_slot).astype(jnp.int32)
    results = []
    for wind in winds:
        folded = fold_quarters(wind, slots, half)
        fourier = jnp.einsum("pjk,pmk->pjm", table_north, folded, precision=HIGH)
        outgoing = fourier.reshape(4, quarter, slots, 2 * local_waves).transpose(1, 2, 0, 3)
        received = lax.all_to_all(outgoing, ("col", "row"), split_axis=0, concat_axis=0, tiled=True)
        shaped = received.reshape(columns, row_devices, block, slots, 4, 2, local_waves)
        arranged = shaped.transpose(1, 3, 5, 2, 4, 0, 6).reshape(
            levels, 2, block * 4, columns * local_waves
        )
        placed = jnp.concatenate(
            [lax.dynamic_slice_in_dim(arranged, holder[level], 1, 0) for level in range(levels)], axis=0
        )
        even = jnp.einsum("lyk,kx->lyx", placed[:, 0], table_east[0], precision=HIGH)
        odd = jnp.einsum("lyk,kx->lyx", placed[:, 1], table_east[1], precision=HIGH)
        total, rest = even + odd, even - odd
        results.append(
            (
                jnp.concatenate([total[:, :, :cells], rest[:, :, :cells]], axis=2),
                jnp.concatenate([total[:, :, cells:], rest[:, :, cells:]], axis=2),
            )
        )
    return results[0][0], results[1][0], results[0][1], results[1][1]


def cos_sin(product, period):
    angles = 2.0 * np.pi * (product % period) / period
    return np.stack([np.cos(angles), np.sin(angles)]).astype(np.float32)


def split(value):
    high = value.astype(jnp.bfloat16)
    return high, (value - high.astype(jnp.float32)).astype(jnp.bfloat16)


def dot3(left, right, dims):
    def one(first, second):
        return lax.dot_general(first, second, (dims, ((), ())), preferred_element_type=jnp.float32)

    return one(left[0], right[0]) + one(left[0], right[1]) + one(left[1], right[0])


def sizes_of(shape, columns, row_devices):
    slots, local, north_cells = shape[1:]
    return dict(
        columns=columns,
        rows=row_devices,
        devices=columns * row_devices,
        slots=slots,
        local=local,
        half=local // 2,
        north=north_cells,
        quarter=north_cells // 4,
        share=north_cells // (columns * row_devices),
        east=2 * local * columns,
        cells=local * columns,
    )


def build_north_table(sz, fine, coarse, table):
    quarter = sz["quarter"]

    def step(g, carry):
        cos_c, sin_c = coarse[0, pl.ds(g, 1), :], coarse[1, pl.ds(g, 1), :]
        cos_f, sin_f = fine[0], fine[1]
        cosine = cos_c * cos_f - sin_c * sin_f
        sine = -(sin_c * cos_f + cos_c * sin_f)
        at = pl.ds(pl.multiple_of(g * FINE, FINE), FINE)
        for part, value in ((0, cosine), (1, sine)):
            high, low = split(value)
            table[0, at, part * quarter:(part + 1) * quarter] = high
            table[1, at, part * quarter:(part + 1) * quarter] = low
        return carry

    lax.fori_loop(0, quarter // FINE, step, 0)


def build_east_table(sz, parity, fine, coarse, table):
    half, columns, cells = sz["half"], sz["columns"], sz["cells"]

    def step(column, carry):
        base = column * (2 * half)
        index = parity * columns + column
        for start in range(0, cells, TILE):
            lanes = slice(start, start + TILE)
            cos_c, sin_c = coarse[0, pl.ds(index, 1), lanes], coarse[1, pl.ds(index, 1), lanes]
            cos_f, sin_f = fine[0, :, lanes], fine[1, :, lanes]
            cosine = cos_c * cos_f - sin_c * sin_f
            sine = -(sin_c * cos_f + cos_c * sin_f)
            for part, value in ((0, cosine), (1, sine)):
                at = pl.ds(pl.multiple_of(base + part * half, half), half)
                high, low = split(value)
                table[0, at, lanes] = high
                table[1, at, lanes] = low
        return carry

    lax.fori_loop(0, columns, step, 0)


def build_folded(sz, slot, wind, parity, column, curl, source, cut, twiddle, folded, ready):
    half, quarter, north = sz["half"], sz["quarter"], sz["north"]
    is_north = wind == 1

    def step(block, carry):
        ready(block)
        lanes = pl.multiple_of(block * LANES, LANES)
        index = lax.broadcasted_iota(jnp.int32, (ROWS, LANES), 1) + lanes
        line = lax.broadcasted_iota(jnp.int32, (ROWS, LANES), 0)
        for top in range(0, half, ROWS):
            at = pl.ds(parity + 2 * top, ROWS, stride=2)
            wave = column * (2 * half) + parity + 2 * (line + top)
            kx = (2.0 * math.pi / sz["east"]) * wave.astype(jnp.float32)
            weight = jnp.where(wave == 0, 1.0, 2.0)
            kept = cut[at, :]
            real, imag = [], []
            for q in range(4):
                number = index + q * quarter
                number = jnp.where(number < north // 2, number, number - north)
                ky = (2.0 * math.pi / north) * number.astype(jnp.float32)
                square = kx * kx + ky * ky
                retained = (jnp.abs(number) <= kept) & (square > 0)
                inverse = jnp.where(retained, weight / jnp.where(square > 0, square, 1.0), 0.0)
                by_x, by_y = kx * inverse, ky * inverse
                first = jnp.where(is_north, by_x, -by_y)
                second = jnp.where(is_north, by_y, by_x)
                strip = block + q * (quarter // LANES)
                zr, zi = curl[slot, strip, 0, at, :], curl[slot, strip, 1, at, :]
                dr, di = source[slot, strip, 0, at, :], source[slot, strip, 1, at, :]
                real.append(first * zi + second * di)
                imag.append(-(first * zr + second * dr))
            (r0, r1, r2, r3), (i0, i1, i2, i3) = real, imag
            rs, rd, rt, ru = r0 + r2, r0 - r2, r1 + r3, r1 - r3
            js, jd, jt, ju = i0 + i2, i0 - i2, i1 + i3, i1 - i3
            parts = ((rs + rt, js + jt), (rd - ju, jd + ru), (rs - rt, js - jt), (rd + ju, jd - ru))
            near = pl.ds(lanes, LANES)
            far = pl.ds(pl.multiple_of(lanes + quarter, LANES), LANES)
            for p, (a, b) in enumerate(parts):
                if p:
                    cosine = twiddle[2 * p:2 * p + 1, near]
                    sine = twiddle[2 * p + 1:2 * p + 2, near]
                    a, b = a * cosine - b * sine, a * sine + b * cosine
                upper = slice(p * 2 * half + top, p * 2 * half + top + ROWS)
                lower = slice(p * 2 * half + half + top, p * 2 * half + half + top + ROWS)
                for level, (x, y) in enumerate(zip(split(a), split(b))):
                    folded[level, upper, near] = x
                    folded[level, upper, far] = y
                    folded[level, lower, near] = y
                    folded[level, lower, far] = -x
        return carry

    lax.fori_loop(0, quarter // LANES, step, 0)


def north_transform(sz, chunk, table, folded, outgoing):
    quarter, pair = sz["quarter"], 2 * LANES
    for p in range(0, 4, 2):
        rows = slice(p * LANES, p * LANES + pair)
        sums = dot3((table[0], table[1]), (folded[0, rows], folded[1, rows]), ((1,), (1,)))
        outgoing[chunk, pl.ds(p, quarter, stride=4), :] = sums[:, :LANES]
        outgoing[chunk, pl.ds(p + 1, quarter, stride=4), :] = sums[:, LANES:]


def build_waves(sz, parity, received, waves):
    columns, half = sz["columns"], sz["half"]
    lines = sz["rows"] * sz["share"]

    def step(column, carry):
        sources = pl.ds(pl.multiple_of(column * sz["rows"], sz["rows"]), sz["rows"])
        lane = lax.broadcasted_iota(jnp.int32, (1, 2 * half), 1)
        into = pl.ds(pl.multiple_of(column * 2 * half, LANES), 2 * half)
        value = received[sources].reshape(lines, 2 * half)
        wave = column * (2 * half) + parity + 2 * jnp.where(lane < half, lane, lane - half)
        kx = (2.0 * math.pi / sz["east"]) * wave.astype(jnp.float32)
        slope = pltpu.roll(value, half, axis=1) * jnp.where(lane < half, -kx, kx)
        for kind, data in enumerate((value, slope)):
            high, low = split(data)
            waves[0, kind * lines:(kind + 1) * lines, into] = high
            waves[1, kind * lines:(kind + 1) * lines, into] = low
        return carry

    lax.fori_loop(0, columns, step, 0)


def east_tile(waves, table, lanes):
    return dot3((waves[0], waves[1]), (table[0, :, lanes], table[1, :, lanes]), ((1,), (0,)))


def exchange_kernel(
    sz, curl_hbm, source_hbm, cut_row, fine_north, coarse_north, twiddle, fine_east, coarse_east,
    results, even, last, table_odd,
    curl, source, cut, table_north, table_even, folded, outgoing, incoming, waves,
    load_sem, send_sem, recv_sem, own_sem,
):
    columns, rows, devices, slots = sz["columns"], sz["rows"], sz["devices"], sz["slots"]
    share, cells, quarter = sz["share"], sz["cells"], sz["quarter"]
    chunks = 4 * slots
    col, row = lax.axis_index("col"), lax.axis_index("row")
    me = col * rows + row
    blocks = quarter // LANES
    strips = 4 * blocks

    def load(slot, strip):
        lanes = pl.ds(pl.multiple_of(strip * LANES, LANES), LANES)
        for which, (hbm, near) in enumerate(((curl_hbm, curl), (source_hbm, source))):
            yield pltpu.make_async_copy(
                hbm.at[:, slot, :, lanes], near.at[slot, strip], load_sem.at[which, slot, strip]
            )

    def start_load(index, carry):
        turn = index % strips
        for copy in load(index // strips, (turn % 4) * blocks + turn // 4):
            copy.start()
        return carry

    lax.fori_loop(0, slots * strips, start_load, 0)
    barrier = pltpu.get_barrier_semaphore()
    itself = columns // 2

    def target(offset):
        there_col = lax.rem(col + itself + offset % columns, columns)
        there_row = lax.rem(row + offset // columns, rows)
        return there_col, there_row

    def origin(offset):
        from_col = lax.rem(col + 2 * columns - itself - offset % columns, columns)
        from_row = lax.rem(row + rows - offset // columns, rows)
        return from_col * rows + from_row

    def others(step):
        lax.fori_loop(0, itself, step, 0)
        lax.fori_loop(itself + 1, devices, step, 0)

    def greet(offset, carry):
        pl.semaphore_signal(barrier, inc=1, device_id=target(offset), device_id_type=MESH)
        return carry

    others(greet)
    cut[...] = jnp.broadcast_to(cut_row[...], (sz["local"], sz["local"])).T
    build_north_table(sz, fine_north, coarse_north, table_north)

    def block_of(device):
        return pl.ds(pl.multiple_of(device * share, share), share)

    def send(chunk, offset, slot_ref):
        there_col, there_row = target(offset)
        return pltpu.make_async_remote_copy(
            src_ref=outgoing.at[chunk, block_of(there_col * rows + there_row)],
            dst_ref=slot_ref,
            send_sem=send_sem.at[chunk, offset],
            recv_sem=recv_sem.at[chunk, offset],
            device_id=(there_col, there_row),
            device_id_type=MESH,
        )

    def own(chunk, slot_ref):
        return pltpu.make_async_copy(outgoing.at[chunk, block_of(me)], slot_ref, own_sem.at[chunk])

    def launch(chunk, arrivals):
        def step(offset, carry):
            send(chunk, offset, arrivals(me)).start()
            return carry

        others(step)
        own(chunk, arrivals(me)).start()

    def collect(chunk, arrivals):
        own(chunk, arrivals(me)).wait()

        def step(offset, carry):
            send(chunk, offset, arrivals(origin(offset))).wait_recv()
            return carry

        others(step)

    def drain(chunk, arrivals):
        def step(offset, carry):
            send(chunk, offset, arrivals(me)).wait_send()
            return carry

        others(step)

    def produce(chunk, carry):
        slot, wind, parity = chunk // 4, (chunk // 2) % 2, chunk % 2

        def ready(block):
            @pl.when(chunk % 4 == 0)
            def _():
                for q in range(4):
                    for copy in load(slot, block + q * blocks):
                        copy.wait()

        build_folded(sz, slot, wind, parity, col, curl, source, cut, twiddle, folded, ready)
        north_transform(sz, chunk, table_north, folded, outgoing)

        @pl.when(chunk == 0)
        def _():
            pl.semaphore_wait(barrier, devices - 1)

        @pl.when(chunk < chunks - 1)
        def _():
            launch(chunk, lambda device: incoming.at[chunk, device])

        @pl.when(chunk == chunks - 1)
        def _():
            launch(chunk, lambda device: last.at[device])

        return carry

    lax.fori_loop(0, chunks, produce, 0)
    build_east_table(sz, 0, fine_east, coarse_east, table_even)
    build_east_table(sz, 1, fine_east, coarse_east, table_odd)

    def consume(chunk, carry):
        collect(chunk, lambda device: incoming.at[chunk, device])
        pair, parity = chunk // 2, chunk % 2
        build_waves(sz, parity, incoming.at[chunk], waves)

        @pl.when(parity == 0)
        def _():
            def tile(index, inner):
                at = pl.ds(pl.multiple_of(index * TILE, TILE), TILE)
                even[:, at] = east_tile(waves, table_even, at)
                return inner

            lax.fori_loop(0, cells // TILE, tile, 0)

        @pl.when(parity == 1)
        def _():
            def tile(index, inner):
                at = pl.ds(pl.multiple_of(index * TILE, TILE), TILE)
                beyond = pl.ds(pl.multiple_of(index * TILE + cells, TILE), TILE)
                odd = east_tile(waves, table_odd, at)
                results[pair, :, at] = even[:, at] + odd
                results[pair, :, beyond] = even[:, at] - odd
                return inner

            lax.fori_loop(0, cells // TILE, tile, 0)

        return carry

    lax.fori_loop(0, chunks - 1, consume, 0)

    def drain_early(chunk, carry):
        drain(chunk, lambda device: incoming.at[chunk, device])
        return carry

    lax.fori_loop(0, chunks - 1, drain_early, 0)
    drain(chunks - 1, lambda device: last.at[device])
    collect(chunks - 1, lambda device: last.at[device])


def finish_kernel(
    sz, level_slot, results, even, last, table_odd, u_wind, v_wind, u_slope, v_slope,
    waves, grid, place_sem, write_sem,
):
    rows, slots, share, cells = sz["rows"], sz["slots"], sz["share"], sz["cells"]
    pairs = 2 * slots
    outs = ((u_wind, v_wind), (u_slope, v_slope))
    pending = []
    spots = [(kind, row) for kind in range(2) for row in range(rows)]

    def spread(source_ref, pair, lanes, sems):
        for index, (kind, row) in enumerate(spots):
            lines = pl.ds(index * share, share)
            level = level_slot[row * slots + pair // 2]
            copy = pltpu.make_async_copy(
                source_ref.at[lines, lanes], outs[kind][pair % 2].at[level, :, lanes], sems.at[index]
            )
            copy.start()
            pending.append(copy)

    for pair in range(pairs - 1):
        spread(results.at[pair], pair, pl.ds(0, 2 * cells), place_sem.at[pair])
    build_waves(sz, 1, last, waves)
    for t in range(cells // TILE):
        odd = east_tile(waves, table_odd, pl.ds(t * TILE, TILE))
        held = even[:, t * TILE:(t + 1) * TILE]
        for part, value in enumerate((held + odd, held - odd)):
            start = part * cells + t * TILE
            grid[:, start:start + TILE] = value
            spread(grid, pairs - 1, pl.ds(start, TILE), write_sem.at[t, part])
    for copy in pending:
        copy.wait()


def on_device(vorticity, divergence, trunc_cut, level_slot):
    columns, row_devices = lax.axis_size("col"), lax.axis_size("row")
    sz = sizes_of(vorticity.shape, columns, row_devices)
    if sz["local"] != LANES or sz["cells"] % 256 or sz["quarter"] % LANES:
        return general_device(vorticity, divergence, trunc_cut, level_slot)
    local, half, quarter, cells = sz["local"], sz["half"], sz["quarter"], sz["cells"]
    devices, slots, share, east = sz["devices"], sz["slots"], sz["share"], sz["east"]
    pairs, chunks, levels = 2 * slots, 4 * slots, slots * row_devices
    strips = sz["north"] // LANES
    lines = 2 * row_devices * share
    column = np.arange(quarter)
    fine_north = cos_sin(np.arange(FINE)[:, None] * column, quarter)
    coarse_north = cos_sin(FINE * np.arange(quarter // FINE)[:, None] * column, quarter)
    twiddle = cos_sin(np.arange(4)[:, None] * column, sz["north"]).transpose(1, 0, 2).reshape(8, quarter)
    cell = np.arange(cells)
    fine_east = cos_sin(2 * np.arange(half)[:, None] * cell, east)
    first = np.arange(2)[:, None] + local * np.arange(columns)[None, :]
    coarse_east = cos_sin(first.reshape(-1, 1) * cell, east)
    f32, bf16 = jnp.float32, jnp.bfloat16
    anywhere = pl.BlockSpec(memory_space=pl.ANY)
    here = pl.BlockSpec(memory_space=pltpu.VMEM)
    results, even, last, table_odd = pl.pallas_call(
        functools.partial(exchange_kernel, sz),
        out_shape=(
            pltpu.VMEM((pairs - 1, lines, east), f32),
            pltpu.VMEM((lines, cells), f32),
            pltpu.VMEM((devices, share, local), f32),
            pltpu.VMEM((2, cells, cells), bf16),
        ),
        in_specs=[anywhere] * 2 + [here] * 6,
        out_specs=(here,) * 4,
        scratch_shapes=[
            pltpu.VMEM((slots, strips, 2, local, LANES), f32),
            pltpu.VMEM((slots, strips, 2, local, LANES), f32),
            pltpu.VMEM((local, LANES), jnp.int32),
            pltpu.VMEM((2, quarter, 2 * quarter), bf16),
            pltpu.VMEM((2, cells, cells), bf16),
            pltpu.VMEM((2, 4 * local, 2 * quarter), bf16),
            pltpu.VMEM((chunks, sz["north"], local), f32),
            pltpu.VMEM((chunks - 1, devices, share, local), f32),
            pltpu.VMEM((2, lines, cells), bf16),
            pltpu.SemaphoreType.DMA((2, slots, strips)),
            pltpu.SemaphoreType.DMA((chunks, devices)),
            pltpu.SemaphoreType.DMA((chunks, devices)),
            pltpu.SemaphoreType.DMA((chunks,)),
        ],
        compiler_params=pltpu.CompilerParams(
            collective_id=0, has_side_effects=True, vmem_limit_bytes=40 * 2**20
        ),
        name="exchange",
    )(
        vorticity, divergence, trunc_cut.reshape(1, local),
        fine_north, coarse_north, twiddle, fine_east, coarse_east,
    )
    out = jax.ShapeDtypeStruct((levels, share, east), f32)
    return pl.pallas_call(
        functools.partial(finish_kernel, sz),
        out_shape=(out,) * 4,
        in_specs=[pl.BlockSpec(memory_space=pltpu.SMEM)] + [here] * 4,
        out_specs=(anywhere,) * 4,
        scratch_shapes=[
            pltpu.VMEM((2, lines, cells), bf16),
            pltpu.VMEM((lines, east), f32),
            pltpu.SemaphoreType.DMA((pairs - 1, 2 * row_devices)),
            pltpu.SemaphoreType.DMA((cells // TILE, 2, 2 * row_devices)),
        ],
        compiler_params=pltpu.CompilerParams(vmem_limit_bytes=16 * 2**20),
        name="finish",
    )(level_slot, results, even, last, table_odd)


def solution(mesh):
    return jax.shard_map(
        on_device,
        mesh=mesh,
        in_specs=(P(None, "row", "col", None), P(None, "row", "col", None), P("col"), P()),
        out_specs=(P(None, ("col", "row"), None),) * 4,
        check_vma=False,
    )
```

```python
import functools
import math

import jax
import jax.numpy as jnp
import numpy as np
from jax import lax
from jax.experimental import pallas as pl
from jax.experimental.pallas import tpu as pltpu
from jax.sharding import PartitionSpec as P

MESH = pl.DeviceIdType.MESH
LANES = 128
ROWS = 16
FINE = 32
TILE = 256
HIGH = lax.Precision.HIGH


def split_waves(array, axis):
    first = lax.slice_in_dim(array, 0, None, 2, axis)
    second = lax.slice_in_dim(array, 1, None, 2, axis)
    return jnp.concatenate([first, second], axis)


def phases(product, period):
    angles = 2.0 * np.pi * (product % period) / period
    return np.cos(angles).astype(np.float32), np.sin(angles).astype(np.float32)


def multiply(first, second):
    return first[0] * second[0] - first[1] * second[1], first[0] * second[1] + first[1] * second[0]


def north_table(north_cells):
    quarter = north_cells // 4
    fine = math.gcd(quarter, 32)
    column = np.arange(quarter)
    coarse_row = 4 * fine * np.arange(quarter // fine)[None, :, None, None] + np.arange(4)[:, None, None, None]
    fine_row = 4 * np.arange(fine)[None, None, :, None]
    coarse = phases(coarse_row * column, north_cells)
    close = phases(fine_row * column, north_cells)
    coarse, close = lax.optimization_barrier((coarse, close))
    cosine, sine = multiply(coarse, close)
    joined = jnp.concatenate([cosine, -sine], axis=3)
    return joined.reshape(4, quarter, 2 * quarter)


def east_table(columns, local_waves, east_cells):
    half = local_waves // 2
    cells = east_cells // 2
    column = np.arange(cells)
    coarse_wave = np.arange(2)[:, None, None, None] + local_waves * np.arange(columns)[None, :, None, None]
    close_wave = 2 * np.arange(half)[None, None, :, None]
    coarse = phases(coarse_wave * column, east_cells)
    close = phases(close_wave * column, east_cells)
    coarse, close = lax.optimization_barrier((coarse, close))
    cosine, sine = multiply(coarse, close)
    wave = coarse_wave + close_wave
    weights = np.where(wave == 0, 1.0, 2.0).astype(np.float32)
    scaled = (weights * wave * (2.0 * np.pi / east_cells)).astype(np.float32)
    real = jnp.concatenate([weights * cosine, -scaled * sine], axis=3)
    imag = jnp.concatenate([-weights * sine, -scaled * cosine], axis=3)
    joined = jnp.stack([real, imag], axis=2)
    return joined.reshape(2, columns * local_waves, 2 * cells)


def spectral_winds(vorticity, divergence, trunc_cut, wave_index, east_cells):
    north_cells = vorticity.shape[3]
    north_index = jnp.arange(north_cells, dtype=jnp.int32)
    north_wave = jnp.where(north_index < north_cells // 2, north_index, north_index - north_cells)
    wave_east = 2.0 * math.pi / east_cells * wave_index.astype(jnp.float32)
    wave_north = 2.0 * math.pi / north_cells * north_wave.astype(jnp.float32)
    east_col = wave_east[:, None]
    north_row = wave_north[None, :]
    square_wave = east_col * east_col + north_row * north_row
    retained = (jnp.abs(north_wave)[None, :] <= trunc_cut[:, None]) & (square_wave > 0)
    inverse_square = jnp.where(retained, 1.0 / jnp.where(square_wave > 0, square_wave, 1.0), 0.0)
    east_inverse = east_col * inverse_square
    north_inverse = north_row * inverse_square
    curl_real, curl_imag = vorticity[0], vorticity[1]
    source_real, source_imag = divergence[0], divergence[1]
    east = (
        -north_inverse * curl_imag + east_inverse * source_imag,
        north_inverse * curl_real - east_inverse * source_real,
    )
    north = (
        east_inverse * curl_imag + north_inverse * source_imag,
        -east_inverse * curl_real - north_inverse * source_real,
    )
    return east, north


def fold_quarters(wind, slots, half):
    real, imag = wind
    quarter = real.shape[2] // 4
    r0, r1, r2, r3 = (real[:, :, q * quarter:(q + 1) * quarter] for q in range(4))
    i0, i1, i2, i3 = (imag[:, :, q * quarter:(q + 1) * quarter] for q in range(4))
    folded = (
        (r0 + r2 + (r1 + r3), i0 + i2 + (i1 + i3)),
        (r0 - r2 - (i1 - i3), i0 - i2 + (r1 - r3)),
        (r0 + r2 - (r1 + r3), i0 + i2 - (i1 + i3)),
        (r0 - r2 + (i1 - i3), i0 - i2 - (r1 - r3)),
    )
    parts = []
    for part_real, part_imag in folded:
        shape = (slots, 2, 1, half, 2 * quarter)
        top = jnp.concatenate([part_real, part_imag], axis=2).reshape(shape)
        low = jnp.concatenate([part_imag, -part_real], axis=2).reshape(shape)
        parts.append(jnp.concatenate([top, low], axis=2))
    return jnp.stack(parts, axis=0).reshape(4, slots * 4 * half, 2 * quarter)


def general_device(vorticity, divergence, trunc_cut, level_slot):
    columns = lax.axis_size("col")
    row_devices = lax.axis_size("row")
    slots, local_waves, north_cells = vorticity.shape[1:]
    half = local_waves // 2
    quarter = north_cells // 4
    levels = slots * row_devices
    east_cells = 2 * local_waves * columns
    cells = east_cells // 2
    block = quarter // (columns * row_devices)
    first_wave = lax.axis_index("col") * local_waves
    wave_index = first_wave + jnp.arange(local_waves, dtype=jnp.int32)
    winds = spectral_winds(
        split_waves(vorticity, 2),
        split_waves(divergence, 2),
        split_waves(trunc_cut, 0),
        split_waves(wave_index, 0),
        east_cells,
    )
    table_north = north_table(north_cells)
    table_east = east_table(columns, local_waves, east_cells)
    holder = jnp.argsort(level_slot).astype(jnp.int32)
    results = []
    for wind in winds:
        folded = fold_quarters(wind, slots, half)
        fourier = jnp.einsum("pjk,pmk->pjm", table_north, folded, precision=HIGH)
        outgoing = fourier.reshape(4, quarter, slots, 2 * local_waves).transpose(1, 2, 0, 3)
        received = lax.all_to_all(outgoing, ("col", "row"), split_axis=0, concat_axis=0, tiled=True)
        shaped = received.reshape(columns, row_devices, block, slots, 4, 2, local_waves)
        arranged = shaped.transpose(1, 3, 5, 2, 4, 0, 6).reshape(
            levels, 2, block * 4, columns * local_waves
        )
        placed = jnp.concatenate(
            [lax.dynamic_slice_in_dim(arranged, holder[level], 1, 0) for level in range(levels)], axis=0
        )
        even = jnp.einsum("lyk,kx->lyx", placed[:, 0], table_east[0], precision=HIGH)
        odd = jnp.einsum("lyk,kx->lyx", placed[:, 1], table_east[1], precision=HIGH)
        total, rest = even + odd, even - odd
        results.append(
            (
                jnp.concatenate([total[:, :, :cells], rest[:, :, :cells]], axis=2),
                jnp.concatenate([total[:, :, cells:], rest[:, :, cells:]], axis=2),
            )
        )
    return results[0][0], results[1][0], results[0][1], results[1][1]


def cos_sin(product, period):
    angles = 2.0 * np.pi * (product % period) / period
    return np.stack([np.cos(angles), np.sin(angles)]).astype(np.float32)


def split(value):
    high = value.astype(jnp.bfloat16)
    return high, (value - high.astype(jnp.float32)).astype(jnp.bfloat16)


def dot3(left, right, dims):
    def one(first, second):
        return lax.dot_general(first, second, (dims, ((), ())), preferred_element_type=jnp.float32)

    return one(left[0], right[0]) + one(left[0], right[1]) + one(left[1], right[0])


def sizes_of(shape, columns, row_devices):
    slots, local, north_cells = shape[1:]
    return dict(
        columns=columns,
        rows=row_devices,
        devices=columns * row_devices,
        slots=slots,
        local=local,
        half=local // 2,
        north=north_cells,
        quarter=north_cells // 4,
        share=north_cells // (columns * row_devices),
        east=2 * local * columns,
        cells=local * columns,
    )


def build_north_table(sz, fine, coarse, table):
    quarter = sz["quarter"]

    def step(g, carry):
        cos_c, sin_c = coarse[0, pl.ds(g, 1), :], coarse[1, pl.ds(g, 1), :]
        cos_f, sin_f = fine[0], fine[1]
        cosine = cos_c * cos_f - sin_c * sin_f
        sine = -(sin_c * cos_f + cos_c * sin_f)
        at = pl.ds(pl.multiple_of(g * FINE, FINE), FINE)
        for part, value in ((0, cosine), (1, sine)):
            high, low = split(value)
            table[0, at, part * quarter:(part + 1) * quarter] = high
            table[1, at, part * quarter:(part + 1) * quarter] = low
        return carry

    lax.fori_loop(0, quarter // FINE, step, 0)


def build_east_table(sz, parity, fine, coarse, table):
    half, columns, cells = sz["half"], sz["columns"], sz["cells"]

    def step(column, carry):
        base = column * (2 * half)
        index = parity * columns + column
        for start in range(0, cells, TILE):
            lanes = slice(start, start + TILE)
            cos_c, sin_c = coarse[0, pl.ds(index, 1), lanes], coarse[1, pl.ds(index, 1), lanes]
            cos_f, sin_f = fine[0, :, lanes], fine[1, :, lanes]
            cosine = cos_c * cos_f - sin_c * sin_f
            sine = -(sin_c * cos_f + cos_c * sin_f)
            for part, value in ((0, cosine), (1, sine)):
                at = pl.ds(pl.multiple_of(base + part * half, half), half)
                high, low = split(value)
                table[0, at, lanes] = high
                table[1, at, lanes] = low
        return carry

    lax.fori_loop(0, columns, step, 0)


def build_folded(sz, slot, wind, parity, column, curl, source, cut, twiddle, folded, ready):
    half, quarter, north = sz["half"], sz["quarter"], sz["north"]
    is_north = wind == 1

    def step(block, carry):
        ready(block)
        lanes = pl.multiple_of(block * LANES, LANES)
        index = lax.broadcasted_iota(jnp.int32, (ROWS, LANES), 1) + lanes
        line = lax.broadcasted_iota(jnp.int32, (ROWS, LANES), 0)
        for top in range(0, half, ROWS):
            at = pl.ds(parity + 2 * top, ROWS, stride=2)
            wave = column * (2 * half) + parity + 2 * (line + top)
            kx = (2.0 * math.pi / sz["east"]) * wave.astype(jnp.float32)
            weight = jnp.where(wave == 0, 1.0, 2.0)
            kept = cut[at, :]
            real, imag = [], []
            for q in range(4):
                number = index + q * quarter
                number = jnp.where(number < north // 2, number, number - north)
                ky = (2.0 * math.pi / north) * number.astype(jnp.float32)
                square = kx * kx + ky * ky
                retained = (jnp.abs(number) <= kept) & (square > 0)
                inverse = jnp.where(retained, weight / jnp.where(square > 0, square, 1.0), 0.0)
                by_x, by_y = kx * inverse, ky * inverse
                first = jnp.where(is_north, by_x, -by_y)
                second = jnp.where(is_north, by_y, by_x)
                strip = block + q * (quarter // LANES)
                zr, zi = curl[slot, strip, 0, at, :], curl[slot, strip, 1, at, :]
                dr, di = source[slot, strip, 0, at, :], source[slot, strip, 1, at, :]
                real.append(first * zi + second * di)
                imag.append(-(first * zr + second * dr))
            (r0, r1, r2, r3), (i0, i1, i2, i3) = real, imag
            rs, rd, rt, ru = r0 + r2, r0 - r2, r1 + r3, r1 - r3
            js, jd, jt, ju = i0 + i2, i0 - i2, i1 + i3, i1 - i3
            parts = ((rs + rt, js + jt), (rd - ju, jd + ru), (rs - rt, js - jt), (rd + ju, jd - ru))
            near = pl.ds(lanes, LANES)
            far = pl.ds(pl.multiple_of(lanes + quarter, LANES), LANES)
            for p, (a, b) in enumerate(parts):
                if p:
                    cosine = twiddle[2 * p:2 * p + 1, near]
                    sine = twiddle[2 * p + 1:2 * p + 2, near]
                    a, b = a * cosine - b * sine, a * sine + b * cosine
                upper = slice(p * 2 * half + top, p * 2 * half + top + ROWS)
                lower = slice(p * 2 * half + half + top, p * 2 * half + half + top + ROWS)
                for level, (x, y) in enumerate(zip(split(a), split(b))):
                    folded[level, upper, near] = x
                    folded[level, upper, far] = y
                    folded[level, lower, near] = y
                    folded[level, lower, far] = -x
        return carry

    lax.fori_loop(0, quarter // LANES, step, 0)


def north_transform(sz, chunk, table, folded, outgoing):
    quarter, pair = sz["quarter"], 2 * LANES
    for p in range(0, 4, 2):
        rows = slice(p * LANES, p * LANES + pair)
        sums = dot3((table[0], table[1]), (folded[0, rows], folded[1, rows]), ((1,), (1,)))
        outgoing[chunk, pl.ds(p, quarter, stride=4), :] = sums[:, :LANES]
        outgoing[chunk, pl.ds(p + 1, quarter, stride=4), :] = sums[:, LANES:]


def build_waves(sz, parity, received, waves):
    columns, half = sz["columns"], sz["half"]
    lines = sz["rows"] * sz["share"]

    def step(column, carry):
        sources = pl.ds(pl.multiple_of(column * sz["rows"], sz["rows"]), sz["rows"])
        lane = lax.broadcasted_iota(jnp.int32, (1, 2 * half), 1)
        into = pl.ds(pl.multiple_of(column * 2 * half, LANES), 2 * half)
        value = received[sources].reshape(lines, 2 * half)
        wave = column * (2 * half) + parity + 2 * jnp.where(lane < half, lane, lane - half)
        kx = (2.0 * math.pi / sz["east"]) * wave.astype(jnp.float32)
        slope = pltpu.roll(value, half, axis=1) * jnp.where(lane < half, -kx, kx)
        for kind, data in enumerate((value, slope)):
            high, low = split(data)
            waves[0, kind * lines:(kind + 1) * lines, into] = high
            waves[1, kind * lines:(kind + 1) * lines, into] = low
        return carry

    lax.fori_loop(0, columns, step, 0)


def east_tile(waves, table, lanes):
    return dot3((waves[0], waves[1]), (table[0, :, lanes], table[1, :, lanes]), ((1,), (0,)))


def exchange_kernel(
    sz, curl_hbm, source_hbm, cut_row, fine_north, coarse_north, twiddle, fine_hbm, coarse_hbm,
    results, even, last, table_odd,
    curl, source, cut, table_north, table_even, folded, outgoing, incoming, waves, fine_east, coarse_east,
    load_sem, send_sem, recv_sem, own_sem, phase_sem,
):
    columns, rows, devices, slots = sz["columns"], sz["rows"], sz["devices"], sz["slots"]
    share, cells, quarter = sz["share"], sz["cells"], sz["quarter"]
    chunks = 4 * slots
    col, row = lax.axis_index("col"), lax.axis_index("row")
    me = col * rows + row
    blocks = quarter // LANES
    strips = 4 * blocks

    def load(slot, strip):
        lanes = pl.ds(pl.multiple_of(strip * LANES, LANES), LANES)
        for which, (hbm, near) in enumerate(((curl_hbm, curl), (source_hbm, source))):
            yield pltpu.make_async_copy(
                hbm.at[:, slot, :, lanes], near.at[slot, strip], load_sem.at[which, slot, strip]
            )

    def start_load(index, carry):
        turn = index % strips
        for copy in load(index // strips, (turn % 4) * blocks + turn // 4):
            copy.start()
        return carry

    barrier = pltpu.get_barrier_semaphore()
    def target(offset):
        there_col = lax.rem(col + offset % columns, columns)
        there_row = lax.rem(row + offset // columns, rows)
        return there_col, there_row

    def origin(offset):
        from_col = lax.rem(col + columns - offset % columns, columns)
        from_row = lax.rem(row + rows - offset // columns, rows)
        return from_col * rows + from_row

    def others(step):
        lax.fori_loop(1, devices, step, 0)

    def greet(offset, carry):
        pl.semaphore_signal(barrier, inc=1, device_id=target(offset), device_id_type=MESH)
        return carry

    others(greet)
    lax.fori_loop(0, slots * strips, start_load, 0)
    phases = [
        pltpu.make_async_copy(hbm, near, phase_sem.at[index])
        for index, (hbm, near) in enumerate(((fine_hbm, fine_east), (coarse_hbm, coarse_east)))
    ]
    for copy in phases:
        copy.start()
    cut[...] = jnp.broadcast_to(cut_row[...], (sz["local"], sz["local"])).T
    build_north_table(sz, fine_north, coarse_north, table_north)

    def block_of(device):
        return pl.ds(pl.multiple_of(device * share, share), share)

    def send(chunk, offset, slot_ref):
        there_col, there_row = target(offset)
        return pltpu.make_async_remote_copy(
            src_ref=outgoing.at[chunk, block_of(there_col * rows + there_row)],
            dst_ref=slot_ref,
            send_sem=send_sem.at[chunk, offset],
            recv_sem=recv_sem.at[chunk, offset],
            device_id=(there_col, there_row),
            device_id_type=MESH,
        )

    def own(chunk, slot_ref):
        return pltpu.make_async_copy(outgoing.at[chunk, block_of(me)], slot_ref, own_sem.at[chunk])

    def launch(chunk, arrivals):
        def step(offset, carry):
            send(chunk, offset, arrivals(me)).start()
            return carry

        others(step)
        own(chunk, arrivals(me)).start()

    def collect(chunk, arrivals):
        own(chunk, arrivals(me)).wait()

        def step(offset, carry):
            send(chunk, offset, arrivals(origin(offset))).wait_recv()
            return carry

        others(step)

    def drain(chunk, arrivals):
        def step(offset, carry):
            send(chunk, offset, arrivals(me)).wait_send()
            return carry

        others(step)

    def produce(chunk, carry):
        slot, wind, parity = chunk // 4, (chunk // 2) % 2, chunk % 2

        def ready(block):
            @pl.when(chunk % 4 == 0)
            def _():
                for q in range(4):
                    for copy in load(slot, block + q * blocks):
                        copy.wait()

        build_folded(sz, slot, wind, parity, col, curl, source, cut, twiddle, folded, ready)
        north_transform(sz, chunk, table_north, folded, outgoing)

        @pl.when(chunk == 0)
        def _():
            pl.semaphore_wait(barrier, devices - 1)

        @pl.when(chunk < chunks - 1)
        def _():
            launch(chunk, lambda device: incoming.at[chunk, device])

        @pl.when(chunk == chunks - 1)
        def _():
            launch(chunk, lambda device: last.at[device])

        return carry

    lax.fori_loop(0, chunks, produce, 0)
    for copy in phases:
        copy.wait()
    build_east_table(sz, 0, fine_east, coarse_east, table_even)
    build_east_table(sz, 1, fine_east, coarse_east, table_odd)

    def consume(chunk, carry):
        collect(chunk, lambda device: incoming.at[chunk, device])
        pair, parity = chunk // 2, chunk % 2
        build_waves(sz, parity, incoming.at[chunk], waves)

        @pl.when(parity == 0)
        def _():
            def tile(index, inner):
                at = pl.ds(pl.multiple_of(index * TILE, TILE), TILE)
                even[:, at] = east_tile(waves, table_even, at)
                return inner

            lax.fori_loop(0, cells // TILE, tile, 0)

        @pl.when(parity == 1)
        def _():
            def tile(index, inner):
                at = pl.ds(pl.multiple_of(index * TILE, TILE), TILE)
                beyond = pl.ds(pl.multiple_of(index * TILE + cells, TILE), TILE)
                odd = east_tile(waves, table_odd, at)
                results[pair, :, at] = even[:, at] + odd
                results[pair, :, beyond] = even[:, at] - odd
                return inner

            lax.fori_loop(0, cells // TILE, tile, 0)

        return carry

    lax.fori_loop(0, chunks - 1, consume, 0)

    def drain_early(chunk, carry):
        drain(chunk, lambda device: incoming.at[chunk, device])
        return carry

    lax.fori_loop(0, chunks - 1, drain_early, 0)
    drain(chunks - 1, lambda device: last.at[device])
    collect(chunks - 1, lambda device: last.at[device])


def finish_kernel(
    sz, level_slot, results, even, last, table_odd, u_wind, v_wind, u_slope, v_slope,
    waves, grid, place_sem, write_sem,
):
    rows, slots, share, cells = sz["rows"], sz["slots"], sz["share"], sz["cells"]
    pairs = 2 * slots
    outs = ((u_wind, v_wind), (u_slope, v_slope))
    pending = []
    spots = [(kind, row) for kind in range(2) for row in range(rows)]

    def spread(source_ref, pair, lanes, sems):
        for index, (kind, row) in enumerate(spots):
            lines = pl.ds(index * share, share)
            level = level_slot[row * slots + pair // 2]
            copy = pltpu.make_async_copy(
                source_ref.at[lines, lanes], outs[kind][pair % 2].at[level, :, lanes], sems.at[index]
            )
            copy.start()
            pending.append(copy)

    for pair in range(pairs - 1):
        spread(results.at[pair], pair, pl.ds(0, 2 * cells), place_sem.at[pair])
    build_waves(sz, 1, last, waves)
    for t in range(cells // TILE):
        odd = east_tile(waves, table_odd, pl.ds(t * TILE, TILE))
        held = even[:, t * TILE:(t + 1) * TILE]
        for part, value in enumerate((held + odd, held - odd)):
            start = part * cells + t * TILE
            grid[:, start:start + TILE] = value
            spread(grid, pairs - 1, pl.ds(start, TILE), write_sem.at[t, part])
    for copy in pending:
        copy.wait()


def on_device(vorticity, divergence, trunc_cut, level_slot):
    columns, row_devices = lax.axis_size("col"), lax.axis_size("row")
    sz = sizes_of(vorticity.shape, columns, row_devices)
    if sz["local"] != LANES or sz["cells"] % 256 or sz["quarter"] % LANES:
        return general_device(vorticity, divergence, trunc_cut, level_slot)
    local, half, quarter, cells = sz["local"], sz["half"], sz["quarter"], sz["cells"]
    devices, slots, share, east = sz["devices"], sz["slots"], sz["share"], sz["east"]
    pairs, chunks, levels = 2 * slots, 4 * slots, slots * row_devices
    strips = sz["north"] // LANES
    lines = 2 * row_devices * share
    column = np.arange(quarter)
    fine_north = cos_sin(np.arange(FINE)[:, None] * column, quarter)
    coarse_north = cos_sin(FINE * np.arange(quarter // FINE)[:, None] * column, quarter)
    twiddle = cos_sin(np.arange(4)[:, None] * column, sz["north"]).transpose(1, 0, 2).reshape(8, quarter)
    cell = np.arange(cells)
    fine_east = cos_sin(2 * np.arange(half)[:, None] * cell, east)
    first = np.arange(2)[:, None] + local * np.arange(columns)[None, :]
    coarse_east = cos_sin(first.reshape(-1, 1) * cell, east)
    f32, bf16 = jnp.float32, jnp.bfloat16
    anywhere = pl.BlockSpec(memory_space=pl.ANY)
    here = pl.BlockSpec(memory_space=pltpu.VMEM)
    results, even, last, table_odd = pl.pallas_call(
        functools.partial(exchange_kernel, sz),
        out_shape=(
            pltpu.VMEM((pairs - 1, lines, east), f32),
            pltpu.VMEM((lines, cells), f32),
            pltpu.VMEM((devices, share, local), f32),
            pltpu.VMEM((2, cells, cells), bf16),
        ),
        in_specs=[anywhere] * 2 + [here] * 4 + [anywhere] * 2,
        out_specs=(here,) * 4,
        scratch_shapes=[
            pltpu.VMEM((slots, strips, 2, local, LANES), f32),
            pltpu.VMEM((slots, strips, 2, local, LANES), f32),
            pltpu.VMEM((local, LANES), jnp.int32),
            pltpu.VMEM((2, quarter, 2 * quarter), bf16),
            pltpu.VMEM((2, cells, cells), bf16),
            pltpu.VMEM((2, 4 * local, 2 * quarter), bf16),
            pltpu.VMEM((chunks, sz["north"], local), f32),
            pltpu.VMEM((chunks - 1, devices, share, local), f32),
            pltpu.VMEM((2, lines, cells), bf16),
            pltpu.VMEM(fine_east.shape, f32),
            pltpu.VMEM(coarse_east.shape, f32),
            pltpu.SemaphoreType.DMA((2, slots, strips)),
            pltpu.SemaphoreType.DMA((chunks, devices)),
            pltpu.SemaphoreType.DMA((chunks, devices)),
            pltpu.SemaphoreType.DMA((chunks,)),
            pltpu.SemaphoreType.DMA((2,)),
        ],
        compiler_params=pltpu.CompilerParams(
            collective_id=0, has_side_effects=True, vmem_limit_bytes=40 * 2**20
        ),
        name="exchange",
    )(
        vorticity, divergence, trunc_cut.reshape(1, local),
        fine_north, coarse_north, twiddle, fine_east, coarse_east,
    )
    out = jax.ShapeDtypeStruct((levels, share, east), f32)
    return pl.pallas_call(
        functools.partial(finish_kernel, sz),
        out_shape=(out,) * 4,
        in_specs=[pl.BlockSpec(memory_space=pltpu.SMEM)] + [here] * 4,
        out_specs=(anywhere,) * 4,
        scratch_shapes=[
            pltpu.VMEM((2, lines, cells), bf16),
            pltpu.VMEM((lines, east), f32),
            pltpu.SemaphoreType.DMA((pairs - 1, 2 * row_devices)),
            pltpu.SemaphoreType.DMA((cells // TILE, 2, 2 * row_devices)),
        ],
        compiler_params=pltpu.CompilerParams(vmem_limit_bytes=16 * 2**20),
        name="finish",
    )(level_slot, results, even, last, table_odd)


def solution(mesh):
    return jax.shard_map(
        on_device,
        mesh=mesh,
        in_specs=(P(None, "row", "col", None), P(None, "row", "col", None), P("col"), P()),
        out_specs=(P(None, ("col", "row"), None),) * 4,
        check_vma=False,
    )
```
